32 devices in a mesh: depth: 16 (over z, y, core), chan: 2 (over x).
Axes of the slice: x: 2, y: 2, z: 4, core: 2. Of those that a mesh axis runs over, the one named last changes fastest.
Arguments:
- pre: float32 [1, 512, 32, 256], P(None, 'chan', 'depth'), may hold values from -6 to 6
- grad_out: float32 [1, 512, 32, 256], P(None, 'chan', 'depth'), may hold values from -6 to 6
- weight: float32 [27, 512, 512], P(None, 'chan'), may hold values from -0.0546875 to 0.0546875
Outputs:
- grad_pre: float32 [1, 512, 32, 256], P(None, 'chan', 'depth')
- grad_weight: float32 [27, 512, 512], P(None, 'chan', 'depth')
The draws below stay inside these ranges and needn't reach their ends.
All inputs are finite; a program needn't handle non-finite values.
Results may differ from the reference program's by a relative error of at most 0.0001.
Values sent between devices are 32-bit elements; how exact they have to be, the bound alone decides.
A program may use at most 192 MiB of HBM per device.

```python
import math
import jax
import jax.numpy as jnp
from jax import lax

C = 512
W = 16
BATCH = 1
PLANE = 256
DEPTH = 32
VOXELS = 8192


def strengthened(result, stream_key, source, target, blocks, factor):
    owner, partner = [(jnp.arange(result.shape[position]) // (result.shape[position] // blocks)).reshape([-1 if axis == position else 1 for axis in range(result.ndim)]) for position in (source, target)]
    chosen = jax.random.permutation(stream_key, blocks)[partner]
    strong = (owner == chosen) | (owner == (partner + blocks // 2) % blocks)
    return jnp.where(strong, factor * result, result)


def shard_levels(stream_key, dims, shards, low, top_value):
    level, own = 1.0, jax.random.fold_in(stream_key, 6)
    for dim, blocks in shards:
        draws = jnp.exp(jax.random.uniform(jax.random.fold_in(own, dim), (blocks,), jnp.float32, low / len(shards), top_value / len(shards)))
        level = level * jnp.repeat(draws, dims[dim] // blocks).reshape([-1 if axis == dim else 1 for axis in range(len(dims))])
    return level


def normal_values(stream_key, extent, width, reach, split=(), kind=jnp.bfloat16):
    drawn = width * jax.random.normal(stream_key, extent, jnp.float32)
    if split:
        drawn = drawn * shard_levels(stream_key, extent, split, -0.22, 0.18)
    return jnp.clip(drawn, -reach, reach).astype(kind)


def gaussian_with(own_key, extent, deviation, reach, pieces, heavy, dtype=jnp.bfloat16):
    entries = deviation * jax.random.normal(own_key, extent, jnp.float32)
    if pieces:
        entries = entries * shard_levels(own_key, extent, pieces, -0.22, 0.18)
    return jnp.clip(strengthened(entries, jax.random.fold_in(own_key, 3), *heavy), -reach, reach).astype(dtype)


def setup_inputs(seed: int = 0) -> dict:
    arg_keys = jax.random.split(jax.random.key(seed), 4)
    pre = normal_values(arg_keys[0], (BATCH, C, DEPTH, PLANE), 1.0, 6.0, ((1, 2), (2, 16)), jnp.float32)
    grad_out = gaussian_with(arg_keys[1], (BATCH, C, DEPTH, PLANE), 1.0, 6.0, ((1, 2), (2, 16)), (2, 1, 16, 2.0), jnp.float32)
    weight = normal_values(arg_keys[2], (27, C, C), (27 * C) ** -0.5, 0.0546875, ((1, 2),), jnp.float32)
    return {"pre": pre, "grad_out": grad_out, "weight": weight}


def shift_plane(block, drow, dcol):
    plane = block.shape[-1]
    step = drow * W + dcol
    lead = [(0, 0)] * (block.ndim - 1)
    if step > 0:
        moved = jnp.pad(block[..., step:], lead + [(0, step)])
    elif step < 0:
        moved = jnp.pad(block[..., :plane + step], lead + [(-step, 0)])
    else:
        moved = block
    column = jnp.arange(plane) % W
    valid = (column + dcol >= 0) & (column + dcol < W)
    return jnp.where(valid, moved, jnp.float32(0.0))

def normal_cdf(value):
    return 0.5 * (1.0 + jax.scipy.special.erf(value / math.sqrt(2.0)))

def reference(pre, grad_out, weight):
    act = pre * normal_cdf(pre)
    depth_pad = [(0, 0), (0, 0), (1, 1), (0, 0)]
    act_pad = jnp.pad(act, depth_pad)
    cot_pad = jnp.pad(grad_out, depth_pad)
    grad_act = jnp.zeros(pre.shape, jnp.float32)
    filters = []
    for depth_off in range(3):
        for row_off in range(3):
            for col_off in range(3):
                index = 9 * depth_off + 3 * row_off + col_off
                source = shift_plane(act_pad[:, :, depth_off:depth_off + DEPTH], row_off - 1, col_off - 1)
                filters.append(jnp.einsum('bcdp,bodp->co', source, grad_out, precision=lax.Precision.HIGHEST))
                moved = shift_plane(cot_pad[:, :, 2 - depth_off:2 - depth_off + DEPTH], 1 - row_off, 1 - col_off)
                grad_act = grad_act + jnp.einsum('co,bodp->bcdp', weight[index], moved, precision=lax.Precision.HIGHEST)
    slope = normal_cdf(pre) + pre * jnp.exp(-0.5 * pre * pre) / math.sqrt(2.0 * math.pi)
    grad_pre = grad_act * slope
    grad_weight = jnp.stack(filters) * float(VOXELS) ** (-0.5)
    return (grad_pre, grad_weight)
```

```python
import functools
import math

import jax
import jax.numpy as jnp
from jax import lax
from jax.experimental import pallas as pl
from jax.experimental.pallas import tpu as pltpu
from jax.sharding import PartitionSpec as P

W = 16
MESH = pl.DeviceIdType.MESH
F32, BF16 = jnp.float32, jnp.bfloat16


def normal_cdf(value):
    return 0.5 * (1.0 + lax.erf(value * (1.0 / math.sqrt(2.0))))


def split(value):
    high = value.astype(BF16)
    return high, (value - high.astype(F32)).astype(BF16)


def moved(value, drow, dcol):
    plane = value.shape[-1]
    lane = lax.broadcasted_iota(jnp.int32, value.shape, value.ndim - 1)
    step = drow * W + dcol
    turned = pltpu.roll(value, lax.rem(plane - step, plane), value.ndim - 1)
    col = lax.rem(lane, W) + dcol
    cell = lane + drow * W
    valid = (col >= 0) & (col < W) & (cell >= 0) & (cell < plane)
    return jnp.where(valid, turned, 0.0)


def dot(a, b):
    return jnp.dot(a, b, preferred_element_type=F32)


def dot_nt(a, b):
    return lax.dot_general(a, b, (((1,), (1,)), ((), ())), preferred_element_type=F32)


def kernel(far, near, scale, pre_ref, g_ref, w_ref, gp_ref, gw_ref,
           act, gs, fr, s_hi, s_lo, v_hi, v_lo, wb, acc, other, ga,
           local, gx_s, gx_r, h_s, h_r, hx_s, hx_r, a_r, a_s, f_s, f_r, t_s, t_r, e_s, e_r, w_sem):
    d, x = lax.axis_index("depth"), lax.axis_index("chan")
    nd, nc = lax.axis_size("depth"), lax.axis_size("chan")
    chips = far * near
    planes, cl, plane = pre_ref.shape
    ob = nc * cl // chips
    oc = ob // 2
    k, chip = lax.rem(d, 2), d // 2
    f, n = chip // near, lax.rem(chip, near)

    def dev(f_, n_, k_=None):
        return ((f_ * near + n_) * 2 + (k if k_ is None else k_), x)

    def remote(src, dst, ss, rs, to):
        return pltpu.make_async_remote_copy(src_ref=src, dst_ref=dst, send_sem=ss, recv_sem=rs, device_id=to, device_id_type=MESH)

    load_g = pltpu.make_async_copy(g_ref, gs.at[x, pl.ds(1, planes)], local.at[0])
    load_g.start()
    load_a = pltpu.make_async_copy(pre_ref, act.at[chip], local.at[1])
    load_a.start()

    bar = pltpu.get_barrier_semaphore()

    def hello(to):
        pl.semaphore_signal(bar, inc=1, device_id=to, device_id_type=MESH)

    for j in range(1, nc):
        hello((d, lax.rem(x + j, nc)))

    def hello_chip(j, carry):
        other_chip = lax.rem(chip + j, chips)
        hello((other_chip * 2 + k, x))
        return carry

    lax.fori_loop(1, chips, hello_chip, 0)
    hello((d + 1 - 2 * k, x))
    outer = d - 1 + 2 * k
    has_outer = (outer >= 0) & (outer < nd)

    @pl.when(has_outer)
    def _():
        hello((outer, x))

    pl.semaphore_wait(bar, nc - 1 + chips + jnp.where(has_outer, 1, 0))

    has = (d > 0, d < nd - 1)
    halo_in = []
    load_g.wait()
    to_next = remote(gs.at[x, planes], gs.at[x, 0], h_s.at[0], h_r.at[0], (d + 1, x))
    to_prev = remote(gs.at[x, 1], gs.at[x, planes + 1], h_s.at[1], h_r.at[1], (d - 1, x))

    @pl.when(has[1])
    def _():
        to_next.start()

    @pl.when(has[0])
    def _():
        to_prev.start()

    def g_send(j):
        to = (d, lax.rem(x + j, nc))
        span = pl.ds(1, planes)
        return remote(gs.at[x, span], gs.at[x, span], gx_s.at[j], gx_r.at[j], to)

    def halo_send(j, side):
        to = (d, lax.rem(x + j, nc))
        row = (0, planes + 1)[side]
        return remote(gs.at[x, row], gs.at[x, row], hx_s.at[j, side], hx_r.at[j, side], to)

    def g_recv(j):
        c = lax.rem(x + nc - j, nc)
        span = pl.ds(1, planes)
        return remote(gs.at[c, span], gs.at[c, span], gx_s.at[j], gx_r.at[j], (d, c))

    def halo_recv(j, side):
        c = lax.rem(x + nc - j, nc)
        row = (0, planes + 1)[side]
        return remote(gs.at[c, row], gs.at[c, row], hx_s.at[j, side], hx_r.at[j, side], (d, c))

    for j in range(1, nc):
        g_send(j).start()

    load_a.wait()

    def a_copy(slot, way, to):
        return remote(act.at[slot], act.at[slot], a_s.at[slot, way], a_r.at[slot], to)

    def a_forward(slot, up, down):
        @pl.when(up)
        def _():
            a_copy(slot, 0, dev(f + 1, n)).start()

        @pl.when(down)
        def _():
            a_copy(slot, 1, dev(f - 1, n)).start()

        for j in range(1, near):
            a_copy(slot, 1 + j, dev(f, lax.rem(n + j, near))).start()

    a_forward(chip, f < far - 1, f > 0)

    def relay(t):
        for sgn in range(2):
            f_ = f + (2 * sgn - 1) * t

            @pl.when((t < far) & (f_ >= 0) & (f_ < far))
            def _():
                slot = f_ * near + n
                a_copy(slot, 0, dev(f, n)).wait_recv()
                if sgn == 0:
                    a_forward(slot, f < far - 1, False)
                else:
                    a_forward(slot, False, f > 0)

    def f_copy(j):
        to_chip = lax.rem(chip + j, chips)
        first = to_chip * ob
        c, off = first // cl, pl.multiple_of(lax.rem(first, cl), ob)
        src = gs.at[c, pl.ds(1, planes), pl.ds(off, ob)]
        return c, remote(src, fr.at[chip, k], f_s.at[j], f_r.at[j], (to_chip * 2 + k, x))

    def f_start(mine):
        def step(j, carry):
            c, copy = f_copy(j)

            @pl.when((c == x) == mine)
            def _():
                copy.start()

            return carry

        lax.fori_loop(1, chips, step, 0)

    f_start(True)

    zero = jnp.zeros((cl, plane), F32)
    for side in range(2):
        @pl.when(jnp.logical_not(has[side]))
        def _():
            for c in range(nc):
                gs[c, (0, planes + 1)[side]] = zero

    ga[...] = jnp.zeros_like(ga)

    steps = nc * 9

    def chan_at(m):
        return lax.rem(x + nc - m, nc)

    def w_copy(step, kd):
        m, v = step // 9, lax.rem(step, 9)
        c, slot = chan_at(m), lax.rem(step, 2)
        src = w_ref.at[9 * kd + v, :, pl.ds(pl.multiple_of(c * cl, cl), cl)] if cl % 128 == 0 else w_ref.at[9 * kd + v]
        return pltpu.make_async_copy(src, wb.at[slot, kd], w_sem.at[slot, kd])

    for kd in range(3):
        w_copy(0, kd).start()

    def grad_act(m):
        c = chan_at(m)

        def body(v, carry):
            step = m * 9 + v
            slot = lax.rem(step, 2)

            @pl.when(step + 1 < steps)
            def _():
                for kd in range(3):
                    w_copy(step + 1, kd).start()

            drow, dcol = 1 - v // 3, 1 - lax.rem(v, 3)
            for q in range(planes + 2):
                hi, lo = split(moved(gs[c, q], drow, dcol))
                v_hi[:, pl.ds(q * plane, plane)] = hi
                v_lo[:, pl.ds(q * plane, plane)] = lo
            for kd in range(3):
                w_copy(step, kd).wait()
            total = None
            for kd in range(3):
                w = wb[slot, kd]
                if cl % 128 != 0:
                    pick = (lax.broadcasted_iota(jnp.int32, (w.shape[1], cl), 0)
                            == lax.broadcasted_iota(jnp.int32, (w.shape[1], cl), 1) + c * cl).astype(BF16)
                    w_hi, w_lo = split(w)
                    w_hi, w_lo = dot(w_hi, pick).astype(BF16), dot(w_lo, pick).astype(BF16)
                else:
                    w_hi, w_lo = split(w)
                span = pl.ds((2 - kd) * plane, planes * plane)
                part = dot(w_hi, v_hi[:, span]) + dot(w_lo, v_hi[:, span]) + dot(w_hi, v_lo[:, span])
                total = part if total is None else total + part
            ga[...] += total
            return carry

        lax.fori_loop(0, 9, body, 0)

    def halo_wait(side, copy):
        @pl.when(has[side])
        def _():
            copy()

    def own_halo(side):
        (to_next, to_prev)[side].wait_recv()
        for j in range(1, nc):
            halo_send(j, side).start()

    for side in range(2):
        halo_wait(side, functools.partial(own_halo, side))
    grad_act(0)
    relay(1)
    for j in range(1, nc):
        g_recv(j).wait_recv()
    f_start(False)
    first = chip * ob
    c0, off0 = first // cl, pl.multiple_of(lax.rem(first, cl), ob)
    mine = gs.at[c0, pl.ds(1, planes), pl.ds(off0, ob)]
    twin = (d + 1 - 2 * k, x)

    def t_copy(s, src):
        return remote(src, fr.at[s, k], t_s.at[s], t_r.at[s], twin)

    t_copy(chip, mine).start()
    for q in range(planes):
        fr[chip, k, q] = gs[c0, 1 + q, pl.ds(off0, ob)]
    for j in range(1, nc):
        for side in range(2):
            halo_wait(side, lambda: halo_recv(j, side).wait_recv())
        grad_act(j)
    own = act[chip]
    for q in range(planes):
        u = own[q]
        slope = normal_cdf(u) + u * jnp.exp(-0.5 * u * u) * (1.0 / math.sqrt(2.0 * math.pi))
        gp_ref[q] = ga[:, pl.ds(q * plane, plane)] * slope
    relay(2)

    def f_arrive(j, carry):
        s = lax.rem(chip + chips - j, chips)
        remote(fr.at[s, k], fr.at[s, k], f_s.at[j], f_r.at[j], (s * 2 + k, x)).wait_recv()
        t_copy(s, fr.at[s, k]).start()
        return carry

    lax.fori_loop(1, chips, f_arrive, 0)

    def t_arrive(s, carry):
        remote(fr.at[s, 1 - k], fr.at[s, 1 - k], t_s.at[s], t_r.at[s], twin).wait_recv()
        return carry

    lax.fori_loop(0, chips, t_arrive, 0)

    rows = 9 * oc
    for edge in (0, nd * planes + 1):
        s_hi[edge] = jnp.zeros(s_hi.shape[1:], BF16)
        s_lo[edge] = jnp.zeros(s_lo.shape[1:], BF16)

    def shifts(i, carry):
        s, c = i // 2, lax.rem(i, 2)
        for q in range(planes):
            block = fr[s, c, q]
            at = i * planes + q + 1
            for v in range(9):
                hi, lo = split(moved(block, 1 - v // 3, 1 - v % 3))
                for h in range(2):
                    s_hi[at, pl.ds(h * rows + v * oc, oc)] = hi[h * oc:(h + 1) * oc]
                    s_lo[at, pl.ds(h * rows + v * oc, oc)] = lo[h * oc:(h + 1) * oc]
        return carry

    lax.fori_loop(0, nd, shifts, 0)
    acc[...] = jnp.zeros_like(acc)

    def filter_block(s):
        parts = []
        for q in range(planes):
            u = act[s, q]
            parts.append(split(u * normal_cdf(u)))
        first_plane = (2 * s + k) * planes

        def body(kd, carry):
            total = None
            for q in range(planes):
                at = first_plane + q - kd + 2
                a_hi, a_lo = parts[q]
                part = dot_nt(s_hi[at], a_hi) + dot_nt(s_lo[at], a_hi) + dot_nt(s_hi[at], a_lo)
                total = part if total is None else total + part
            acc[kd] += total
            return carry

        for kd in range(3):
            body(kd, 0)

    def distance(t, carry):
        @pl.when(t >= 1)
        def _():
            relay(t + 2)

        def candidate(i, inner):
            j, sgn = i // 2, lax.rem(i, 2)
            dist = t - jnp.where(j > 0, 1, 0)
            f_ = f + (2 * sgn - 1) * dist
            valid = (dist >= 0) & (dist < far) & (f_ >= 0) & (f_ < far) & ((dist > 0) | (sgn == 0))

            @pl.when(valid)
            def _():
                slot = f_ * near + lax.rem(n + j, near)

                @pl.when(j > 0)
                def _():
                    a_copy(slot, 0, dev(f, n)).wait_recv()

                filter_block(slot)

            return inner

        lax.fori_loop(0, 2 * near, candidate, 0)
        return carry

    lax.fori_loop(0, far + 1, distance, 0)

    swap = remote(acc.at[:, pl.ds(pl.multiple_of((1 - k) * rows, rows), rows)], other, e_s.at[0], e_r.at[0], twin)
    swap.start()

    for j in range(1, nc):
        g_send(j).wait_send()
        for side in range(2):
            halo_wait(side, lambda: halo_send(j, side).wait_send())
    halo_wait(1, lambda: to_next.wait_send())
    halo_wait(0, lambda: to_prev.wait_send())

    def f_left(j, carry):
        f_copy(j)[1].wait_send()
        return carry

    lax.fori_loop(1, chips, f_left, 0)

    def t_left(s, carry):
        t_copy(s, fr.at[s, k]).wait_send()
        return carry

    lax.fori_loop(0, chips, t_left, 0)

    def a_left(f_, carry):
        slot = f_ * near + n

        @pl.when((f_ <= f) & (f < far - 1))
        def _():
            a_copy(slot, 0, dev(f + 1, n)).wait_send()

        @pl.when((f_ >= f) & (f > 0))
        def _():
            a_copy(slot, 1, dev(f - 1, n)).wait_send()

        for j in range(1, near):
            a_copy(slot, 1 + j, dev(f, lax.rem(n + j, near))).wait_send()
        return carry

    lax.fori_loop(0, far, a_left, 0)
    swap.wait()
    gw_ref[...] = (acc[:, pl.ds(pl.multiple_of(k * rows, rows), rows)] + other[...]) * scale


def shards(pre, grad_out, weight):
    batch, cl, planes, plane = pre.shape
    nd, nc = lax.axis_size("depth"), lax.axis_size("chan")
    chips = nd // 2
    far = math.gcd(chips, 4)
    near = chips // far
    outs = weight.shape[2]
    ob = outs // chips
    oc = ob // 2
    scale = float(batch * planes * nd * plane) ** (-0.5)
    cut = cl if cl % 128 == 0 else outs
    any_spec = pl.BlockSpec(memory_space=pl.ANY)
    vmem = pl.BlockSpec(memory_space=pltpu.VMEM)
    dma = pltpu.SemaphoreType.DMA
    rows = 9 * ob
    gp, gw = pl.pallas_call(
        functools.partial(kernel, far, near, scale),
        out_shape=(
            jax.ShapeDtypeStruct((planes, cl, plane), F32),
            jax.ShapeDtypeStruct((3, 9 * oc, cl), F32),
        ),
        in_specs=[any_spec, any_spec, any_spec],
        out_specs=(vmem, vmem),
        scratch_shapes=[
            pltpu.VMEM((chips, planes, cl, plane), F32),
            pltpu.VMEM((nc, planes + 2, cl, plane), F32),
            pltpu.VMEM((chips, 2, planes, ob, plane), F32),
            pltpu.VMEM((nd * planes + 2, rows, plane), BF16),
            pltpu.VMEM((nd * planes + 2, rows, plane), BF16),
            pltpu.VMEM((cl, (planes + 2) * plane), BF16),
            pltpu.VMEM((cl, (planes + 2) * plane), BF16),
            pltpu.VMEM((2, 3, cl, cut), F32),
            pltpu.VMEM((3, rows, cl), F32),
            pltpu.VMEM((3, 9 * oc, cl), F32),
            pltpu.VMEM((cl, planes * plane), F32),
            dma((2,)),
            dma((nc,)), dma((nc,)),
            dma((2,)), dma((2,)),
            dma((nc, 2)), dma((nc, 2)),
            dma((chips,)), dma((chips, 1 + near)),
            dma((chips,)), dma((chips,)),
            dma((chips,)), dma((chips,)),
            dma((1,)), dma((1,)),
            dma((2, 3)),
        ],
        compiler_params=pltpu.CompilerParams(
            collective_id=0, has_side_effects=True, vmem_limit_bytes=60 * 1024 * 1024
        ),
    )(pre[0].transpose(1, 0, 2), grad_out[0].transpose(1, 0, 2), weight)
    grad_pre = gp.transpose(1, 0, 2)[None]
    grad_weight = gw.reshape(27, oc, cl).transpose(0, 2, 1)
    return (grad_pre, grad_weight)


def solution(mesh):
    placed = (P(None, "chan", "depth", None), P(None, "chan", "depth", None), P(None, "chan", None))
    return jax.shard_map(
        shards,
        mesh=mesh,
        in_specs=placed,
        out_specs=(P(None, "chan", "depth", None), P(None, "chan", "depth")),
        check_vma=False,
    )
```

```python
import functools
import math

import jax
import jax.numpy as jnp
from jax import lax
from jax.experimental import pallas as pl
from jax.experimental.pallas import tpu as pltpu
from jax.sharding import PartitionSpec as P

W = 16
MESH = pl.DeviceIdType.MESH
F32, BF16 = jnp.float32, jnp.bfloat16


def normal_cdf(value):
    return 0.5 * (1.0 + lax.erf(value * (1.0 / math.sqrt(2.0))))


def split(value):
    high = value.astype(BF16)
    return high, (value - high.astype(F32)).astype(BF16)


def moved(value, drow, dcol):
    plane = value.shape[-1]
    lane = lax.broadcasted_iota(jnp.int32, value.shape, value.ndim - 1)
    step = drow * W + dcol
    turned = pltpu.roll(value, lax.rem(plane - step, plane), value.ndim - 1)
    col = lax.rem(lane, W) + dcol
    cell = lane + drow * W
    valid = (col >= 0) & (col < W) & (cell >= 0) & (cell < plane)
    return jnp.where(valid, turned, 0.0)


def dot(a, b):
    return jnp.dot(a, b, preferred_element_type=F32)


def dot_nt(a, b):
    return lax.dot_general(a, b, (((1,), (1,)), ((), ())), preferred_element_type=F32)


def kernel(far, near, share, scale, pre_ref, g_ref, w_ref, gp_ref, gw_ref,
           act, gs, fr, s_hi, s_lo, v_hi, v_lo, wb, acc, other, ga,
           local, gx_s, gx_r, h_s, h_r, hx_s, hx_r, a_r, a_s, f_s, f_r, fx_s, fx_r, t_s, t_r, e_s, e_r, w_sem):
    d, x = lax.axis_index("depth"), lax.axis_index("chan")
    nd, nc = lax.axis_size("depth"), lax.axis_size("chan")
    chips = far * near
    planes, cl, plane = pre_ref.shape
    ob = nc * cl // chips
    oc = ob // 2
    k, chip = lax.rem(d, 2), d // 2
    f, n = chip // near, lax.rem(chip, near)

    def dev(f_, n_, k_=None):
        return ((f_ * near + n_) * 2 + (k if k_ is None else k_), x)

    def remote(src, dst, ss, rs, to):
        return pltpu.make_async_remote_copy(src_ref=src, dst_ref=dst, send_sem=ss, recv_sem=rs, device_id=to, device_id_type=MESH)

    twin = (d + 1 - 2 * k, x)

    load_g = pltpu.make_async_copy(g_ref, gs.at[x, pl.ds(1, planes)], local.at[0])
    load_g.start()
    load_a = pltpu.make_async_copy(pre_ref, act.at[chip], local.at[1])
    load_a.start()

    bar = pltpu.get_barrier_semaphore()

    def hello(to):
        pl.semaphore_signal(bar, inc=1, device_id=to, device_id_type=MESH)

    for j in range(1, nc):
        hello((d, lax.rem(x + j, nc)))

    def hello_chip(j, carry):
        other_chip = lax.rem(chip + j, chips)
        hello((other_chip * 2 + k, x))
        return carry

    lax.fori_loop(1, chips, hello_chip, 0)
    hello((d + 1 - 2 * k, x))
    outer = d - 1 + 2 * k
    has_outer = (outer >= 0) & (outer < nd)

    @pl.when(has_outer)
    def _():
        hello((outer, x))

    pl.semaphore_wait(bar, nc - 1 + chips + jnp.where(has_outer, 1, 0))

    has = (d > 0, d < nd - 1)
    load_g.wait()
    to_next = remote(gs.at[x, planes], gs.at[x, 0], h_s.at[0], h_r.at[0], (d + 1, x))
    to_prev = remote(gs.at[x, 1], gs.at[x, planes + 1], h_s.at[1], h_r.at[1], (d - 1, x))

    @pl.when(has[1])
    def _():
        to_next.start()

    @pl.when(has[0])
    def _():
        to_prev.start()

    def g_send(j):
        to = (d, lax.rem(x + j, nc))
        span = pl.ds(1, planes)
        return remote(gs.at[x, span], gs.at[x, span], gx_s.at[j], gx_r.at[j], to)

    def halo_outer(j, receive):
        row = k * (planes + 1)
        c = lax.rem(x + nc - j, nc) if receive else x
        to = (d, c if receive else lax.rem(x + j, nc))
        return remote(gs.at[c, row], gs.at[c, row], hx_s.at[j, 0], hx_r.at[j, 0], to)

    def halo_inner(j, receive):
        c = lax.rem(x + nc - j, nc)
        dst = gs.at[c, (1 - k if receive else k) * (planes + 1)]
        src = dst if receive else gs.at[c, planes - k * (planes - 1)]
        return remote(src, dst, hx_s.at[j, 1], hx_r.at[j, 1], twin)

    def g_recv(j):
        c = lax.rem(x + nc - j, nc)
        span = pl.ds(1, planes)
        return remote(gs.at[c, span], gs.at[c, span], gx_s.at[j], gx_r.at[j], (d, c))

    for j in range(1, nc):
        g_send(j).start()

    load_a.wait()

    def a_copy(slot, q, way, to):
        return remote(act.at[slot, q], act.at[slot, q], a_s.at[slot, q, way], a_r.at[slot, q], to)

    last = planes - 1
    low, high = f == 0, f == far - 1
    low_next, high_next = (f == 1) & (far >= 4), (f == far - 2) & (far >= 4)

    def column_sends(f_, q, run):
        slot = f_ * near + n
        ways = [
            ((f_ <= f) & (f < far - 1), 0, dev(f + 1, n)),
            ((f_ >= f) & (f > 0), 1, dev(f - 1, n)),
        ]
        around = (low_next & (f_ == 0)) | (high_next & (f_ == far - 1))
        if q == last:
            around = around | ((far >= 4) & ((low & (f_ == 1)) | (high & (f_ == far - 2))))
        for j in range(1, near):
            ways.append((jnp.logical_not(around), 1 + j, dev(f, lax.rem(n + j, near))))
        for cond, way, to in ways:
            @pl.when(cond)
            def _():
                run(a_copy(slot, q, way, to))

    def layer_sends(j, q, run, late):
        slot = f * near + lax.rem(n + j, near)
        up, down = (high_next, low_next) if late else (low & (far >= 4), high & (far >= 4))

        @pl.when(up)
        def _():
            run(a_copy(slot, q, 0, dev(f + 1, n)))

        @pl.when(down)
        def _():
            run(a_copy(slot, q, 1, dev(f - 1, n)))

    def start(copy):
        copy.start()

    def left(copy):
        copy.wait_send()

    for q in range(planes):
        column_sends(f, q, start)

    def relay(t, q):
        for sgn in range(2):
            f_ = f + (2 * sgn - 1) * t

            @pl.when((t < far) & (f_ >= 0) & (f_ < far))
            def _():
                a_copy(f_ * near + n, q, 0, dev(f, n)).wait_recv()
                column_sends(f_, q, start)

    def relay_layer(q):
        for j in range(1, near):
            a_copy(f * near + lax.rem(n + j, near), q, 0, dev(f, n)).wait_recv()
            layer_sends(j, q, start, False)

    sub = ob // share
    part, base = lax.rem(x, share), x - lax.rem(x, share)

    def f_copy(j):
        to_chip = lax.rem(chip + j, chips)
        at = to_chip * ob + part * sub
        c, off = at // cl, pl.multiple_of(lax.rem(at, cl), sub)
        src = gs.at[c, pl.ds(1, planes), pl.ds(off, sub)]
        dst = fr.at[chip, k, :, pl.ds(pl.multiple_of(part * sub, sub), sub)]
        return c, remote(src, dst, f_s.at[j], f_r.at[j], (to_chip * 2 + k, x))

    def f_start(mine):
        def step(j, carry):
            c, copy = f_copy(j)

            @pl.when((c == x) == mine)
            def _():
                copy.start()

            return carry

        lax.fori_loop(1, chips, step, 0)

    f_start(True)

    zero = jnp.zeros((cl, plane), F32)
    for side in range(2):
        @pl.when(jnp.logical_not(has[side]))
        def _():
            for c in range(nc):
                gs[c, (0, planes + 1)[side]] = zero

    ga[...] = jnp.zeros_like(ga)

    steps = nc * 9

    def chan_at(m):
        return lax.rem(x + nc - m, nc)

    def w_copy(step, kd):
        m, v = step // 9, lax.rem(step, 9)
        c, slot = chan_at(m), lax.rem(step, 2)
        src = w_ref.at[9 * kd + v, :, pl.ds(pl.multiple_of(c * cl, cl), cl)] if cl % 128 == 0 else w_ref.at[9 * kd + v]
        return pltpu.make_async_copy(src, wb.at[slot, kd], w_sem.at[slot, kd])

    for kd in range(3):
        w_copy(0, kd).start()

    def grad_act(m, begin, end):
        c = chan_at(m)

        def body(v, carry):
            step = m * 9 + v
            slot = lax.rem(step, 2)

            @pl.when(step + 1 < steps)
            def _():
                for kd in range(3):
                    w_copy(step + 1, kd).start()

            drow, dcol = 1 - v // 3, 1 - lax.rem(v, 3)
            for q in range(planes + 2):
                hi, lo = split(moved(gs[c, q], drow, dcol))
                v_hi[:, pl.ds(q * plane, plane)] = hi
                v_lo[:, pl.ds(q * plane, plane)] = lo
            for kd in range(3):
                w_copy(step, kd).wait()
            total = None
            for kd in range(3):
                w = wb[slot, kd]
                if cl % 128 != 0:
                    pick = (lax.broadcasted_iota(jnp.int32, (w.shape[1], cl), 0)
                            == lax.broadcasted_iota(jnp.int32, (w.shape[1], cl), 1) + c * cl).astype(BF16)
                    w_hi, w_lo = split(w)
                    w_hi, w_lo = dot(w_hi, pick).astype(BF16), dot(w_lo, pick).astype(BF16)
                else:
                    w_hi, w_lo = split(w)
                span = pl.ds((2 - kd) * plane, planes * plane)
                part = dot(w_hi, v_hi[:, span]) + dot(w_lo, v_hi[:, span]) + dot(w_hi, v_lo[:, span])
                total = part if total is None else total + part
            ga[...] += total
            return carry

        lax.fori_loop(begin, end, body, 0)

    def halo_wait(side, copy):
        @pl.when(has[side])
        def _():
            copy()

    for side in range(2):
        halo_wait(side, (to_next, to_prev)[side].wait_recv)

    @pl.when(has_outer)
    def _():
        for j in range(1, nc):
            halo_outer(j, False).start()

    grad_act(0, 0, 2)
    relay_layer(0)
    relay(1, 0)
    grad_act(0, 2, 6)
    for q in range(1, planes):
        relay_layer(q)
        relay(1, q)
    for j in range(1, nc):
        g_recv(j).wait_recv()
        halo_inner(j, False).start()
    f_start(False)
    grad_act(0, 6, 9)
    first = chip * ob
    c0, off0 = first // cl, pl.multiple_of(lax.rem(first, cl), ob)
    mine = gs.at[c0, pl.ds(1, planes), pl.ds(off0, ob)]

    def t_copy(s, src):
        return remote(src, fr.at[s, k], t_s.at[s], t_r.at[s], twin)

    t_copy(chip, mine).start()
    for q in range(planes):
        fr[chip, k, q] = gs[c0, 1 + q, pl.ds(off0, ob)]
    for j in range(1, nc):
        @pl.when(has_outer)
        def _():
            halo_outer(j, True).wait_recv()

        halo_inner(j, True).wait_recv()
    grad_act(1, 0, 3)
    relay(2, 0)
    grad_act(1, 3, 7)
    for q in range(1, planes):
        relay(2, q)
    for j in range(1, near):
        layer_sends(j, last, start, True)
    grad_act(1, 7, 9)
    for j in range(2, nc):
        grad_act(j, 0, 9)
    own = act[chip]
    for q in range(planes):
        u = own[q]
        slope = normal_cdf(u) + u * jnp.exp(-0.5 * u * u) * (1.0 / math.sqrt(2.0 * math.pi))
        gp_ref[q] = ga[:, pl.ds(q * plane, plane)] * slope

    def f_share(j, i):
        src = fr.at[lax.rem(chip + chips - j, chips), k, :, pl.ds(pl.multiple_of(part * sub, sub), sub)]
        return remote(src, src, fx_s.at[j, i], fx_r.at[j, i], (d, base + lax.rem(part + i, share)))

    def f_shared(j, i):
        theirs = lax.rem(part + share - i, share)
        dst = fr.at[lax.rem(chip + chips - j, chips), k, :, pl.ds(pl.multiple_of(theirs * sub, sub), sub)]
        return remote(dst, dst, fx_s.at[j, i], fx_r.at[j, i], (d, base + theirs))

    def f_arrive(j, carry):
        src = fr.at[lax.rem(chip + chips - j, chips), k, :, pl.ds(pl.multiple_of(part * sub, sub), sub)]
        remote(src, src, f_s.at[j], f_r.at[j], (d, x)).wait_recv()
        for i in range(1, share):
            f_share(j, i).start()
        return carry

    lax.fori_loop(1, chips, f_arrive, 0)

    def x_arrive(j, carry):
        for i in range(1, share):
            f_shared(j, i).wait_recv()
        s = lax.rem(chip + chips - j, chips)
        t_copy(s, fr.at[s, k]).start()
        return carry

    lax.fori_loop(1, chips, x_arrive, 0)

    def t_arrive(s, carry):
        remote(fr.at[s, 1 - k], fr.at[s, 1 - k], t_s.at[s], t_r.at[s], twin).wait_recv()
        return carry

    lax.fori_loop(0, chips, t_arrive, 0)

    rows = 9 * oc
    for edge in (0, nd * planes + 1):
        s_hi[edge] = jnp.zeros(s_hi.shape[1:], BF16)
        s_lo[edge] = jnp.zeros(s_lo.shape[1:], BF16)

    def shifts(i, carry):
        s, c = i // 2, lax.rem(i, 2)
        for q in range(planes):
            block = fr[s, c, q]
            at = i * planes + q + 1
            for v in range(9):
                hi, lo = split(moved(block, 1 - v // 3, 1 - v % 3))
                for h in range(2):
                    s_hi[at, pl.ds(h * rows + v * oc, oc)] = hi[h * oc:(h + 1) * oc]
                    s_lo[at, pl.ds(h * rows + v * oc, oc)] = lo[h * oc:(h + 1) * oc]
        return carry

    lax.fori_loop(0, nd, shifts, 0)
    acc[...] = jnp.zeros_like(acc)

    def filter_block(s):
        parts = []
        for q in range(planes):
            u = act[s, q]
            parts.append(split(u * normal_cdf(u)))
        first_plane = (2 * s + k) * planes

        def body(kd, carry):
            total = None
            for q in range(planes):
                at = first_plane + q - kd + 2
                a_hi, a_lo = parts[q]
                part = dot_nt(s_hi[at], a_hi) + dot_nt(s_lo[at], a_hi) + dot_nt(s_hi[at], a_lo)
                total = part if total is None else total + part
            acc[kd] += total
            return carry

        for kd in range(3):
            body(kd, 0)

    def distance(t, carry):
        @pl.when(t >= 2)
        def _():
            for q in range(planes):
                relay(t + 2, q)

        def candidate(i, inner):
            j, sgn = i // 2, lax.rem(i, 2)
            dist = t - jnp.where(j > 0, 1, 0)
            f_ = f + (2 * sgn - 1) * dist
            valid = (dist >= 0) & (dist < far) & (f_ >= 0) & (f_ < far) & ((dist > 0) | (sgn == 0))

            @pl.when(valid)
            def _():
                slot = f_ * near + lax.rem(n + j, near)

                @pl.when((j > 0) & (dist > 0))
                def _():
                    for q in range(planes):
                        a_copy(slot, q, 0, dev(f, n)).wait_recv()

                filter_block(slot)

            return inner

        lax.fori_loop(0, 2 * near, candidate, 0)
        return carry

    lax.fori_loop(0, 1, distance, 0)
    relay(3, 0)
    lax.fori_loop(1, 2, distance, 0)
    for q in range(1, planes):
        relay(3, q)
    lax.fori_loop(2, far + 1, distance, 0)

    swap = remote(acc.at[:, pl.ds(pl.multiple_of((1 - k) * rows, rows), rows)], other, e_s.at[0], e_r.at[0], twin)
    swap.start()

    for j in range(1, nc):
        g_send(j).wait_send()
        halo_inner(j, False).wait_send()

        @pl.when(has_outer)
        def _():
            halo_outer(j, False).wait_send()
    halo_wait(1, lambda: to_next.wait_send())
    halo_wait(0, lambda: to_prev.wait_send())

    def f_left(j, carry):
        f_copy(j)[1].wait_send()
        for i in range(1, share):
            f_share(j, i).wait_send()
        return carry

    lax.fori_loop(1, chips, f_left, 0)

    def t_left(s, carry):
        t_copy(s, fr.at[s, k]).wait_send()
        return carry

    lax.fori_loop(0, chips, t_left, 0)

    def a_left(f_, carry):
        for q in range(planes):
            column_sends(f_, q, left)
        return carry

    lax.fori_loop(0, far, a_left, 0)
    for q in range(planes):
        for j in range(1, near):
            layer_sends(j, q, left, False)
            if q == last:
                layer_sends(j, q, left, True)
    swap.wait()
    gw_ref[...] = (acc[:, pl.ds(pl.multiple_of(k * rows, rows), rows)] + other[...]) * scale


def shards(pre, grad_out, weight):
    batch, cl, planes, plane = pre.shape
    nd, nc = lax.axis_size("depth"), lax.axis_size("chan")
    chips = nd // 2
    far = math.gcd(chips, 4)
    near = chips // far
    outs = weight.shape[2]
    ob = outs // chips
    oc = ob // 2
    share = math.gcd(nc, max(ob // 8, 1))
    scale = float(batch * planes * nd * plane) ** (-0.5)
    cut = cl if cl % 128 == 0 else outs
    any_spec = pl.BlockSpec(memory_space=pl.ANY)
    vmem = pl.BlockSpec(memory_space=pltpu.VMEM)
    dma = pltpu.SemaphoreType.DMA
    rows = 9 * ob
    gp, gw = pl.pallas_call(
        functools.partial(kernel, far, near, share, scale),
        out_shape=(
            jax.ShapeDtypeStruct((planes, cl, plane), F32),
            jax.ShapeDtypeStruct((3, 9 * oc, cl), F32),
        ),
        in_specs=[any_spec, any_spec, any_spec],
        out_specs=(vmem, vmem),
        scratch_shapes=[
            pltpu.VMEM((chips, planes, cl, plane), F32),
            pltpu.VMEM((nc, planes + 2, cl, plane), F32),
            pltpu.VMEM((chips, 2, planes, ob, plane), F32),
            pltpu.VMEM((nd * planes + 2, rows, plane), BF16),
            pltpu.VMEM((nd * planes + 2, rows, plane), BF16),
            pltpu.VMEM((cl, (planes + 2) * plane), BF16),
            pltpu.VMEM((cl, (planes + 2) * plane), BF16),
            pltpu.VMEM((2, 3, cl, cut), F32),
            pltpu.VMEM((3, rows, cl), F32),
            pltpu.VMEM((3, 9 * oc, cl), F32),
            pltpu.VMEM((cl, planes * plane), F32),
            dma((2,)),
            dma((nc,)), dma((nc,)),
            dma((2,)), dma((2,)),
            dma((nc, 2)), dma((nc, 2)),
            dma((chips, planes)), dma((chips, planes, 1 + near)),
            dma((chips,)), dma((chips,)),
            dma((chips, share)), dma((chips, share)),
            dma((chips,)), dma((chips,)),
            dma((1,)), dma((1,)),
            dma((2, 3)),
        ],
        compiler_params=pltpu.CompilerParams(
            collective_id=0, has_side_effects=True, vmem_limit_bytes=60 * 1024 * 1024
        ),
    )(pre[0].transpose(1, 0, 2), grad_out[0].transpose(1, 0, 2), weight)
    grad_pre = gp.transpose(1, 0, 2)[None]
    grad_weight = gw.reshape(27, oc, cl).transpose(0, 2, 1)
    return (grad_pre, grad_weight)


def solution(mesh):
    placed = (P(None, "chan", "depth", None), P(None, "chan", "depth", None), P(None, "chan", None))
    return jax.shard_map(
        shards,
        mesh=mesh,
        in_specs=placed,
        out_specs=(P(None, "chan", "depth", None), P(None, "chan", "depth")),
        check_vma=False,
    )
```

```python
import functools
import math

import jax
import jax.numpy as jnp
from jax import lax
from jax.experimental import pallas as pl
from jax.experimental.pallas import tpu as pltpu
from jax.sharding import PartitionSpec as P

W = 16
MESH = pl.DeviceIdType.MESH
F32, BF16 = jnp.float32, jnp.bfloat16


def normal_cdf(value):
    return 0.5 * (1.0 + lax.erf(value * (1.0 / math.sqrt(2.0))))


def split(value):
    high = value.astype(BF16)
    return high, (value - high.astype(F32)).astype(BF16)


def moved(value, drow, dcol):
    plane = value.shape[-1]
    lane = lax.broadcasted_iota(jnp.int32, value.shape, value.ndim - 1)
    step = drow * W + dcol
    turned = pltpu.roll(value, lax.rem(plane - step, plane), value.ndim - 1)
    col = lax.rem(lane, W) + dcol
    cell = lane + drow * W
    valid = (col >= 0) & (col < W) & (cell >= 0) & (cell < plane)
    return jnp.where(valid, turned, 0.0)


def dot(a, b):
    return jnp.dot(a, b, preferred_element_type=F32)


def dot_nt(a, b):
    return lax.dot_general(a, b, (((1,), (1,)), ((), ())), preferred_element_type=F32)


def kernel(far, near, share, scale, pre_ref, g_ref, w_ref, gp_ref, gw_ref,
           act, gs, fr, s_hi, s_lo, v_hi, v_lo, wb, acc, other, ga,
           local, gx_s, gx_r, h_s, h_r, hx_s, hx_r, a_r, a_s, f_s, f_r, fx_s, fx_r, t_s, t_r, e_s, e_r, w_sem):
    d, x = lax.axis_index("depth"), lax.axis_index("chan")
    nd, nc = lax.axis_size("depth"), lax.axis_size("chan")
    chips = far * near
    planes, cl, plane = pre_ref.shape
    ob = nc * cl // chips
    oc = ob // 2
    k, chip = lax.rem(d, 2), d // 2
    f, n = chip // near, lax.rem(chip, near)

    def dev(f_, n_, k_=None):
        return ((f_ * near + n_) * 2 + (k if k_ is None else k_), x)

    def remote(src, dst, ss, rs, to):
        return pltpu.make_async_remote_copy(src_ref=src, dst_ref=dst, send_sem=ss, recv_sem=rs, device_id=to, device_id_type=MESH)

    twin = (d + 1 - 2 * k, x)

    load_g = pltpu.make_async_copy(g_ref, gs.at[x, pl.ds(1, planes)], local.at[0])
    load_g.start()
    load_a = pltpu.make_async_copy(pre_ref, act.at[chip], local.at[1])
    load_a.start()

    bar = pltpu.get_barrier_semaphore()

    def hello(to):
        pl.semaphore_signal(bar, inc=1, device_id=to, device_id_type=MESH)

    for j in range(1, nc):
        hello((d, lax.rem(x + j, nc)))

    def hello_chip(j, carry):
        other_chip = lax.rem(chip + j, chips)
        hello((other_chip * 2 + k, x))
        return carry

    lax.fori_loop(1, chips, hello_chip, 0)
    hello((d + 1 - 2 * k, x))
    outer = d - 1 + 2 * k
    has_outer = (outer >= 0) & (outer < nd)

    @pl.when(has_outer)
    def _():
        hello((outer, x))

    pl.semaphore_wait(bar, nc - 1 + chips + jnp.where(has_outer, 1, 0))

    has = (d > 0, d < nd - 1)
    load_g.wait()
    to_next = remote(gs.at[x, planes], gs.at[x, 0], h_s.at[0], h_r.at[0], (d + 1, x))
    to_prev = remote(gs.at[x, 1], gs.at[x, planes + 1], h_s.at[1], h_r.at[1], (d - 1, x))

    @pl.when(has[1])
    def _():
        to_next.start()

    @pl.when(has[0])
    def _():
        to_prev.start()

    def g_send(j):
        to = (d, lax.rem(x + j, nc))
        span = pl.ds(1, planes)
        return remote(gs.at[x, span], gs.at[x, span], gx_s.at[j], gx_r.at[j], to)

    def halo_outer(j, receive):
        row = k * (planes + 1)
        c = lax.rem(x + nc - j, nc) if receive else x
        to = (d, c if receive else lax.rem(x + j, nc))
        return remote(gs.at[c, row], gs.at[c, row], hx_s.at[j, 0], hx_r.at[j, 0], to)

    def halo_inner(j, receive):
        c = lax.rem(x + nc - j, nc)
        dst = gs.at[c, (1 - k if receive else k) * (planes + 1)]
        src = dst if receive else gs.at[c, planes - k * (planes - 1)]
        return remote(src, dst, hx_s.at[j, 1], hx_r.at[j, 1], twin)

    def g_recv(j):
        c = lax.rem(x + nc - j, nc)
        span = pl.ds(1, planes)
        return remote(gs.at[c, span], gs.at[c, span], gx_s.at[j], gx_r.at[j], (d, c))

    for j in range(1, nc):
        g_send(j).start()

    sub = ob // share
    part, base = lax.rem(x, share), x - lax.rem(x, share)

    def f_copy(j):
        to_chip = lax.rem(chip + j, chips)
        at = to_chip * ob + part * sub
        c, off = at // cl, pl.multiple_of(lax.rem(at, cl), sub)
        src = gs.at[c, pl.ds(1, planes), pl.ds(off, sub)]
        dst = fr.at[chip, k, :, pl.ds(pl.multiple_of(part * sub, sub), sub)]
        return c, remote(src, dst, f_s.at[j], f_r.at[j], (to_chip * 2 + k, x))

    def f_start(mine):
        def step(j, carry):
            c, copy = f_copy(j)

            @pl.when((c == x) == mine)
            def _():
                copy.start()

            return carry

        lax.fori_loop(1, chips, step, 0)

    load_a.wait()

    def a_copy(slot, q, way, to):
        return remote(act.at[slot, q], act.at[slot, q], a_s.at[slot, q, way], a_r.at[slot, q], to)

    last = planes - 1
    low, high = f == 0, f == far - 1
    low_next, high_next = (f == 1) & (far >= 4), (f == far - 2) & (far >= 4)

    def column_sends(f_, q, run):
        slot = f_ * near + n
        ways = [
            ((f_ <= f) & (f < far - 1), 0, dev(f + 1, n)),
            ((f_ >= f) & (f > 0), 1, dev(f - 1, n)),
        ]
        around = (low_next & (f_ == 0)) | (high_next & (f_ == far - 1))
        if q == last:
            around = around | ((far >= 4) & ((low & (f_ == 1)) | (high & (f_ == far - 2))))
        for j in range(1, near):
            ways.append((jnp.logical_not(around), 1 + j, dev(f, lax.rem(n + j, near))))
        for cond, way, to in ways:
            @pl.when(cond)
            def _():
                run(a_copy(slot, q, way, to))

    def layer_sends(j, q, run, late):
        slot = f * near + lax.rem(n + j, near)
        up, down = (high_next, low_next) if late else (low & (far >= 4), high & (far >= 4))

        @pl.when(up)
        def _():
            run(a_copy(slot, q, 0, dev(f + 1, n)))

        @pl.when(down)
        def _():
            run(a_copy(slot, q, 1, dev(f - 1, n)))

    def start(copy):
        copy.start()

    def left(copy):
        copy.wait_send()

    f_start(True)
    for q in range(planes):
        column_sends(f, q, start)

    def relay(t, q):
        for sgn in range(2):
            f_ = f + (2 * sgn - 1) * t

            @pl.when((t < far) & (f_ >= 0) & (f_ < far))
            def _():
                a_copy(f_ * near + n, q, 0, dev(f, n)).wait_recv()
                column_sends(f_, q, start)

    def relay_layer(q):
        for j in range(1, near):
            a_copy(f * near + lax.rem(n + j, near), q, 0, dev(f, n)).wait_recv()
            layer_sends(j, q, start, False)

    zero = jnp.zeros((cl, plane), F32)
    for side in range(2):
        @pl.when(jnp.logical_not(has[side]))
        def _():
            for c in range(nc):
                gs[c, (0, planes + 1)[side]] = zero

    ga[...] = jnp.zeros_like(ga)

    steps = nc * 9

    def chan_at(m):
        return lax.rem(x + nc - m, nc)

    def w_copy(step, kd):
        m, v = step // 9, lax.rem(step, 9)
        c, slot = chan_at(m), lax.rem(step, 2)
        src = w_ref.at[9 * kd + v, :, pl.ds(pl.multiple_of(c * cl, cl), cl)] if cl % 128 == 0 else w_ref.at[9 * kd + v]
        return pltpu.make_async_copy(src, wb.at[slot, kd], w_sem.at[slot, kd])

    for kd in range(3):
        w_copy(0, kd).start()

    def grad_act(m, begin, end):
        c = chan_at(m)

        def body(v, carry):
            step = m * 9 + v
            slot = lax.rem(step, 2)

            @pl.when(step + 1 < steps)
            def _():
                for kd in range(3):
                    w_copy(step + 1, kd).start()

            drow, dcol = 1 - v // 3, 1 - lax.rem(v, 3)
            for q in range(planes + 2):
                hi, lo = split(moved(gs[c, q], drow, dcol))
                v_hi[:, pl.ds(q * plane, plane)] = hi
                v_lo[:, pl.ds(q * plane, plane)] = lo
            for kd in range(3):
                w_copy(step, kd).wait()
            total = None
            for kd in range(3):
                w = wb[slot, kd]
                if cl % 128 != 0:
                    pick = (lax.broadcasted_iota(jnp.int32, (w.shape[1], cl), 0)
                            == lax.broadcasted_iota(jnp.int32, (w.shape[1], cl), 1) + c * cl).astype(BF16)
                    w_hi, w_lo = split(w)
                    w_hi, w_lo = dot(w_hi, pick).astype(BF16), dot(w_lo, pick).astype(BF16)
                else:
                    w_hi, w_lo = split(w)
                span = pl.ds((2 - kd) * plane, planes * plane)
                part = dot(w_hi, v_hi[:, span]) + dot(w_lo, v_hi[:, span]) + dot(w_hi, v_lo[:, span])
                total = part if total is None else total + part
            ga[...] += total
            return carry

        lax.fori_loop(begin, end, body, 0)

    def halo_wait(side, copy):
        @pl.when(has[side])
        def _():
            copy()

    for side in range(2):
        halo_wait(side, (to_next, to_prev)[side].wait_recv)

    @pl.when(has_outer)
    def _():
        for j in range(1, nc):
            halo_outer(j, False).start()

    grad_act(0, 0, 2)
    relay_layer(0)
    relay(1, 0)
    grad_act(0, 2, 6)
    for j in range(1, nc):
        g_recv(j).wait_recv()
        halo_inner(j, False).start()
    f_start(False)
    for q in range(1, planes):
        relay_layer(q)
        relay(1, q)
    grad_act(0, 6, 9)
    first = chip * ob
    c0, off0 = first // cl, pl.multiple_of(lax.rem(first, cl), ob)
    mine = gs.at[c0, pl.ds(1, planes), pl.ds(off0, ob)]

    def t_copy(s, src):
        return remote(src, fr.at[s, k], t_s.at[s], t_r.at[s], twin)

    t_copy(chip, mine).start()
    for q in range(planes):
        fr[chip, k, q] = gs[c0, 1 + q, pl.ds(off0, ob)]
    for j in range(1, nc):
        @pl.when(has_outer)
        def _():
            halo_outer(j, True).wait_recv()

        halo_inner(j, True).wait_recv()
    grad_act(1, 0, 3)
    relay(2, 0)
    grad_act(1, 3, 7)
    for q in range(1, planes):
        relay(2, q)
    for j in range(1, near):
        layer_sends(j, last, start, True)
    def f_share(j, i):
        src = fr.at[lax.rem(chip + chips - j, chips), k, :, pl.ds(pl.multiple_of(part * sub, sub), sub)]
        return remote(src, src, fx_s.at[j, i], fx_r.at[j, i], (d, base + lax.rem(part + i, share)))

    def f_shared(j, i):
        theirs = lax.rem(part + share - i, share)
        dst = fr.at[lax.rem(chip + chips - j, chips), k, :, pl.ds(pl.multiple_of(theirs * sub, sub), sub)]
        return remote(dst, dst, fx_s.at[j, i], fx_r.at[j, i], (d, base + theirs))

    def f_arrive(j, carry):
        src = fr.at[lax.rem(chip + chips - j, chips), k, :, pl.ds(pl.multiple_of(part * sub, sub), sub)]
        remote(src, src, f_s.at[j], f_r.at[j], (d, x)).wait_recv()
        for i in range(1, share):
            f_share(j, i).start()
        return carry

    lax.fori_loop(1, chips, f_arrive, 0)

    def x_arrive(j, carry):
        for i in range(1, share):
            f_shared(j, i).wait_recv()
        s = lax.rem(chip + chips - j, chips)
        t_copy(s, fr.at[s, k]).start()
        return carry

    lax.fori_loop(1, chips, x_arrive, 0)

    grad_act(1, 7, 9)
    for j in range(2, nc):
        grad_act(j, 0, 9)
    own = act[chip]
    for q in range(planes):
        u = own[q]
        slope = normal_cdf(u) + u * jnp.exp(-0.5 * u * u) * (1.0 / math.sqrt(2.0 * math.pi))
        gp_ref[q] = ga[:, pl.ds(q * plane, plane)] * slope

    def t_arrive(s, carry):
        remote(fr.at[s, 1 - k], fr.at[s, 1 - k], t_s.at[s], t_r.at[s], twin).wait_recv()
        return carry

    lax.fori_loop(0, chips, t_arrive, 0)

    rows = 9 * oc
    for edge in (0, nd * planes + 1):
        s_hi[edge] = jnp.zeros(s_hi.shape[1:], BF16)
        s_lo[edge] = jnp.zeros(s_lo.shape[1:], BF16)

    def shifts(i, carry):
        s, c = i // 2, lax.rem(i, 2)
        for q in range(planes):
            block = fr[s, c, q]
            at = i * planes + q + 1
            for v in range(9):
                hi, lo = split(moved(block, 1 - v // 3, 1 - v % 3))
                for h in range(2):
                    s_hi[at, pl.ds(h * rows + v * oc, oc)] = hi[h * oc:(h + 1) * oc]
                    s_lo[at, pl.ds(h * rows + v * oc, oc)] = lo[h * oc:(h + 1) * oc]
        return carry

    lax.fori_loop(0, nd, shifts, 0)
    acc[...] = jnp.zeros_like(acc)

    def filter_block(s):
        parts = []
        for q in range(planes):
            u = act[s, q]
            parts.append(split(u * normal_cdf(u)))
        first_plane = (2 * s + k) * planes

        def body(kd, carry):
            total = None
            for q in range(planes):
                at = first_plane + q - kd + 2
                a_hi, a_lo = parts[q]
                part = dot_nt(s_hi[at], a_hi) + dot_nt(s_lo[at], a_hi) + dot_nt(s_hi[at], a_lo)
                total = part if total is None else total + part
            acc[kd] += total
            return carry

        for kd in range(3):
            body(kd, 0)

    def distance(t, carry):
        @pl.when(t >= 2)
        def _():
            for q in range(planes):
                relay(t + 2, q)

        def candidate(i, inner):
            j, sgn = i // 2, lax.rem(i, 2)
            dist = t - jnp.where(j > 0, 1, 0)
            f_ = f + (2 * sgn - 1) * dist
            valid = (dist >= 0) & (dist < far) & (f_ >= 0) & (f_ < far) & ((dist > 0) | (sgn == 0))

            @pl.when(valid)
            def _():
                slot = f_ * near + lax.rem(n + j, near)

                @pl.when((j > 0) & (dist > 0))
                def _():
                    for q in range(planes):
                        a_copy(slot, q, 0, dev(f, n)).wait_recv()

                filter_block(slot)

            return inner

        lax.fori_loop(0, 2 * near, candidate, 0)
        return carry

    lax.fori_loop(0, 1, distance, 0)
    relay(3, 0)
    lax.fori_loop(1, 2, distance, 0)
    for q in range(1, planes):
        relay(3, q)
    lax.fori_loop(2, far + 1, distance, 0)

    swap = remote(acc.at[:, pl.ds(pl.multiple_of((1 - k) * rows, rows), rows)], other, e_s.at[0], e_r.at[0], twin)
    swap.start()

    for j in range(1, nc):
        g_send(j).wait_send()
        halo_inner(j, False).wait_send()

        @pl.when(has_outer)
        def _():
            halo_outer(j, False).wait_send()
    halo_wait(1, lambda: to_next.wait_send())
    halo_wait(0, lambda: to_prev.wait_send())

    def f_left(j, carry):
        f_copy(j)[1].wait_send()
        for i in range(1, share):
            f_share(j, i).wait_send()
        return carry

    lax.fori_loop(1, chips, f_left, 0)

    def t_left(s, carry):
        t_copy(s, fr.at[s, k]).wait_send()
        return carry

    lax.fori_loop(0, chips, t_left, 0)

    def a_left(f_, carry):
        for q in range(planes):
            column_sends(f_, q, left)
        return carry

    lax.fori_loop(0, far, a_left, 0)
    for q in range(planes):
        for j in range(1, near):
            layer_sends(j, q, left, False)
            if q == last:
                layer_sends(j, q, left, True)
    swap.wait()
    gw_ref[...] = (acc[:, pl.ds(pl.multiple_of(k * rows, rows), rows)] + other[...]) * scale


def shards(pre, grad_out, weight):
    batch, cl, planes, plane = pre.shape
    nd, nc = lax.axis_size("depth"), lax.axis_size("chan")
    chips = nd // 2
    far = math.gcd(chips, 4)
    near = chips // far
    outs = weight.shape[2]
    ob = outs // chips
    oc = ob // 2
    share = math.gcd(nc, max(ob // 8, 1))
    scale = float(batch * planes * nd * plane) ** (-0.5)
    cut = cl if cl % 128 == 0 else outs
    any_spec = pl.BlockSpec(memory_space=pl.ANY)
    vmem = pl.BlockSpec(memory_space=pltpu.VMEM)
    dma = pltpu.SemaphoreType.DMA
    rows = 9 * ob
    gp, gw = pl.pallas_call(
        functools.partial(kernel, far, near, share, scale),
        out_shape=(
            jax.ShapeDtypeStruct((planes, cl, plane), F32),
            jax.ShapeDtypeStruct((3, 9 * oc, cl), F32),
        ),
        in_specs=[any_spec, any_spec, any_spec],
        out_specs=(vmem, vmem),
        scratch_shapes=[
            pltpu.VMEM((chips, planes, cl, plane), F32),
            pltpu.VMEM((nc, planes + 2, cl, plane), F32),
            pltpu.VMEM((chips, 2, planes, ob, plane), F32),
            pltpu.VMEM((nd * planes + 2, rows, plane), BF16),
            pltpu.VMEM((nd * planes + 2, rows, plane), BF16),
            pltpu.VMEM((cl, (planes + 2) * plane), BF16),
            pltpu.VMEM((cl, (planes + 2) * plane), BF16),
            pltpu.VMEM((2, 3, cl, cut), F32),
            pltpu.VMEM((3, rows, cl), F32),
            pltpu.VMEM((3, 9 * oc, cl), F32),
            pltpu.VMEM((cl, planes * plane), F32),
            dma((2,)),
            dma((nc,)), dma((nc,)),
            dma((2,)), dma((2,)),
            dma((nc, 2)), dma((nc, 2)),
            dma((chips, planes)), dma((chips, planes, 1 + near)),
            dma((chips,)), dma((chips,)),
            dma((chips, share)), dma((chips, share)),
            dma((chips,)), dma((chips,)),
            dma((1,)), dma((1,)),
            dma((2, 3)),
        ],
        compiler_params=pltpu.CompilerParams(
            collective_id=0, has_side_effects=True, vmem_limit_bytes=60 * 1024 * 1024
        ),
    )(pre[0].transpose(1, 0, 2), grad_out[0].transpose(1, 0, 2), weight)
    grad_pre = gp.transpose(1, 0, 2)[None]
    grad_weight = gw.reshape(27, oc, cl).transpose(0, 2, 1)
    return (grad_pre, grad_weight)


def solution(mesh):
    placed = (P(None, "chan", "depth", None), P(None, "chan", "depth", None), P(None, "chan", None))
    return jax.shard_map(
        shards,
        mesh=mesh,
        in_specs=placed,
        out_specs=(P(None, "chan", "depth", None), P(None, "chan", "depth")),
        check_vma=False,
    )
```
